32 devices in a mesh: groups: 2 (over x), expert: 16 (over z, y, core).
Axes of the slice: x: 2, y: 2, z: 4, core: 2. Of those that a mesh axis runs over, the one named last changes fastest.
Arguments:
- query_features: bfloat16 [4096, 1024], P(('groups', 'expert')), parts along dimension 0, may hold values from -6 to 6
- query_job_label: int32 [4096], P(('groups', 'expert')), parts along dimension 0, may hold values from 0 to 7, as said below
- selected_specialists: int32 [4096, 2], P(('groups', 'expert')), parts along dimension 0, may hold values from 0 to 8, as said below
- whole_number_mixing_factors: int32 [4096, 2], P(('groups', 'expert')), parts along dimension 0, may hold values from 1 to 8
- copy_room_sizes: int32 [16], replicated, may hold values from 256 to 384, as said below
- first_layer_matrix: bfloat16 [16, 1024, 2048], P('expert'), as said below
- second_layer_matrix: bfloat16 [16, 2048, 1024], P('expert'), as said below
Outputs:
- mixture: bfloat16 [4096, 1024], P(('groups', 'expert')), parts along dimension 0
The draws below stay inside these ranges and needn't reach their ends.
There are 2 independent parts, one for each index of `groups`. The reference program is written for one: setup_inputs(seed, part) draws one part's arguments, and reference() takes and returns one part's arrays. A program takes and returns all parts, laid end to end along the dimension named above; an argument that names none is the same for every part. Nothing has to cross between parts.
Inputs may be any that keep to these rules, and one draw needn't show every extreme that they name: `query_job_label`: each request's task number; column 0 of `selected_specialists` names a task expert of this task. `selected_specialists`: column 0 names a task expert of the row's task (number r from 8 on is task expert r - 8), column 1 a shared expert (below 8). From the rows of one device at most 32 entries go to one expert copy, and in every draw some copy receives exactly 32 entries from every device. `copy_room_sizes`: some copy has capacity 384 and some copy 2 * 128. `first_layer_matrix`: the 1 copies of one shared expert hold equal weights. `second_layer_matrix`: the 1 copies of one shared expert hold equal weights.
All inputs are finite; a program needn't handle non-finite values.
Results may differ from the reference program's by a relative error of at most 0.0058.
Values may be sent and summed in bfloat16 or wider, within the bound.
A program may use at most 64 MiB of HBM per device.

```python
import jax
import jax.numpy as jnp
from jax import lax

D = 1024
HIDDEN_SIZE = 2048
TASKS = 8
SHARED = 8
TOP = 2
ROWS_DEV = 128
EXPERTS = 16
REPL = 1
TASK_EXP = 1
SLOT = 32
CAPACITY = 384
ROWS = 2048


def pick_tickets(device_key, popular, hottest, wanted, slots):
    tickets = popular.shape[0] * slots
    owners = jnp.arange(tickets, dtype=jnp.int32) // slots
    jitter = jax.random.randint(jax.random.fold_in(device_key, 1), (tickets,), 0, 16384)
    scores = jitter + popular[owners] + jnp.where(owners == hottest, 1 << 20, 0)
    ranking = jnp.argsort(-scores, stable=True)
    chosen = owners[ranking[:wanted]]
    shuffled = jax.random.permutation(jax.random.fold_in(device_key, 2), wanted)
    return chosen[shuffled]


def routing_plan(key):
    base_key = jax.random.fold_in(key, 11)
    task_copies = TASKS * TASK_EXP
    group_rows = ROWS_DEV // REPL
    task_popular = jax.random.randint(jax.random.fold_in(base_key, 1), (task_copies,), 0, 8192)
    task_hottest = jax.random.randint(jax.random.fold_in(base_key, 2), (), 0, task_copies)
    shared_popular = jax.random.randint(jax.random.fold_in(base_key, 3), (SHARED,), 0, 8192)
    shared_hottest = jax.random.randint(jax.random.fold_in(base_key, 4), (), 0, SHARED)
    task_base = jax.random.fold_in(base_key, 5)
    shared_base = jax.random.fold_in(base_key, 6)

    def task_device(device):
        return pick_tickets(jax.random.fold_in(task_base, device), task_popular, task_hottest, ROWS_DEV, SLOT)

    def shared_group(group):
        return pick_tickets(jax.random.fold_in(shared_base, group), shared_popular, shared_hottest, group_rows, SLOT)
    task_choice = jax.vmap(task_device)(jnp.arange(EXPERTS, dtype=jnp.int32)).reshape(ROWS)
    shared_choice = jax.vmap(shared_group)(jnp.arange(EXPERTS * REPL, dtype=jnp.int32))
    shared_flat = shared_choice.reshape(EXPERTS, REPL, group_rows).transpose(0, 2, 1).reshape(ROWS)
    tasks = (task_choice // TASK_EXP).astype(jnp.int32)
    numbers = SHARED + task_choice % TASK_EXP
    routing = jnp.stack([numbers, shared_flat], axis=1).astype(jnp.int32)
    return (tasks, routing)


def draw_query_job_label(key, part):
    return routing_plan(key)[0]


def draw_selected_specialists(key, part):
    return routing_plan(key)[1]


def draw_copy_room_sizes(key, part):
    values = jax.random.randint(jax.random.fold_in(key, 1), (EXPERTS,), 2 * ROWS_DEV, CAPACITY + 1)
    top_at = jax.random.randint(jax.random.fold_in(key, 2), (), 0, EXPERTS)
    low_at = (top_at + jax.random.randint(jax.random.fold_in(key, 3), (), 1, EXPERTS)) % EXPERTS
    indices = jnp.arange(EXPERTS, dtype=jnp.int32)
    values = jnp.where(indices == top_at, CAPACITY, values)
    values = jnp.where(indices == low_at, 2 * ROWS_DEV, values)
    return values.astype(jnp.int32)


def copied_weights(key, rows_in, cols_out):
    task_copies = TASKS * TASK_EXP
    shared_part = jax.random.normal(jax.random.fold_in(key, 1), (SHARED, rows_in, cols_out), jnp.float32)
    task_part = jax.random.normal(jax.random.fold_in(key, 2), (task_copies, rows_in, cols_out), jnp.float32)
    stacked = jnp.concatenate([jnp.repeat(shared_part, REPL, axis=0), task_part], axis=0)
    return (stacked * rows_in ** (-0.5)).astype(jnp.bfloat16)


def draw_first_layer_matrix(key, part):
    return copied_weights(jax.random.fold_in(key, 21), D, HIDDEN_SIZE)


def draw_second_layer_matrix(key, part):
    return copied_weights(jax.random.fold_in(key, 22), HIDDEN_SIZE, D)


def place_ends(array, key, least, top_value):
    longest = array.shape.index(max(array.shape))
    spots = []
    for shift in (0, 1):
        where = [jax.random.randint(jax.random.fold_in(key, axis), (), 0, length) for axis, length in enumerate(array.shape)]
        where[longest] = (where[longest] + shift) % array.shape[longest]
        spots.append(tuple(where))
    return array.at[spots[0]].set(least).at[spots[1]].set(top_value)


def block_scale(stream_key, extent, split, smallest, largest):
    def one(position, shards_of):
        draws = jax.random.uniform(jax.random.fold_in(jax.random.fold_in(stream_key, 6), position), (shards_of,), jnp.float32, smallest / len(split), largest / len(split))
        return jnp.repeat(jnp.exp(draws), extent[position] // shards_of).reshape((-1,) + (1,) * (len(extent) - position - 1))

    loudness = one(*split[0])
    for cut in split[1:]:
        loudness = loudness * one(*cut)
    return loudness


def noise(stream_key, shape, deviation, limit, split=(), kind=jnp.bfloat16):
    array = deviation * jax.random.normal(stream_key, shape, jnp.float32)
    if split:
        array = array * block_scale(stream_key, shape, split, -0.22, 0.18)
    return jnp.clip(array, -limit, limit).astype(kind)


def setup_inputs(seed: int = 0, part: int = 0) -> dict:
    splits = jax.random.split(jax.random.key(seed), 8)
    part_splits = jax.random.split(jax.random.fold_in(splits[7], part), 8)
    return {
        "query_features": noise(part_splits[0], (ROWS, D), 1.0, 6.0, ((0, 16),)),
        "query_job_label": draw_query_job_label(jax.random.fold_in(jax.random.fold_in(splits[7], part), 71), part),
        "selected_specialists": draw_selected_specialists(jax.random.fold_in(jax.random.fold_in(splits[7], part), 71), part),
        "whole_number_mixing_factors": place_ends(jax.random.randint(part_splits[3], (ROWS, TOP), 1, 9), jax.random.fold_in(part_splits[3], 1), 1, 8).astype(jnp.int32),
        "copy_room_sizes": draw_copy_room_sizes(jax.random.fold_in(splits[7], 71), part),
        "first_layer_matrix": draw_first_layer_matrix(jax.random.fold_in(splits[7], 71), part),
        "second_layer_matrix": draw_second_layer_matrix(jax.random.fold_in(splits[7], 71), part),
    }


def expert_mlp(block_rows, up_matrix, down_matrix):
    hidden = jax.nn.gelu(jnp.dot(block_rows, up_matrix, preferred_element_type=jnp.float32)).astype(jnp.bfloat16)
    return jnp.dot(hidden, down_matrix, preferred_element_type=jnp.float32).astype(jnp.bfloat16)


def reference(query_features, query_job_label, selected_specialists, whole_number_mixing_factors, copy_room_sizes, first_layer_matrix, second_layer_matrix):
    row_index = jnp.arange(ROWS, dtype=jnp.int32)
    shared_copy = selected_specialists * REPL + (row_index % REPL)[:, None]
    task_copy = SHARED * REPL + query_job_label[:, None] * TASK_EXP + selected_specialists - SHARED
    expert_ids = jnp.where(selected_specialists < SHARED, shared_copy, task_copy).astype(jnp.int32)
    linear_specialist_number = expert_ids.reshape(-1)
    specialist_onehot = (linear_specialist_number[:, None] == jnp.arange(EXPERTS, dtype=jnp.int32)[None, :]).astype(jnp.int32)
    before = jnp.cumsum(specialist_onehot, axis=0) - specialist_onehot
    arrival_rank = jnp.sum(before * specialist_onehot, axis=1).astype(jnp.int32)
    surviving_slot_flags = arrival_rank < copy_room_sizes[linear_specialist_number]
    row_of_entry = (jnp.arange(linear_specialist_number.shape[0], dtype=jnp.int32) // TOP).astype(jnp.int32)

    def one_expert(expert_index):
        target = jnp.where((linear_specialist_number == expert_index) & surviving_slot_flags, arrival_rank, CAPACITY).astype(jnp.int32)
        source = jnp.zeros((CAPACITY,), jnp.int32).at[target].set(row_of_entry, mode="drop")
        live_mask = jnp.zeros((CAPACITY,), jnp.bool_).at[target].set(True, mode="drop")
        block_rows = jnp.where(live_mask[:, None], query_features[source], jnp.zeros((), jnp.bfloat16))
        return expert_mlp(block_rows, first_layer_matrix[expert_index], second_layer_matrix[expert_index])

    outputs = lax.map(one_expert, jnp.arange(EXPERTS, dtype=jnp.int32))
    picked = outputs[linear_specialist_number, jnp.minimum(arrival_rank, CAPACITY - 1)]
    gate_float = whole_number_mixing_factors.astype(jnp.float32)
    gate_share = gate_float / jnp.sum(gate_float, axis=1, keepdims=True)
    row_weight = gate_share.reshape(-1) * surviving_slot_flags.astype(jnp.float32)
    weighted = row_weight[:, None] * picked.astype(jnp.float32)
    return jnp.sum(weighted.reshape(ROWS, TOP, D), axis=1).astype(jnp.bfloat16)
```

```python
import functools

import jax
import jax.numpy as jnp
from jax import lax
from jax.experimental import pallas as pl
from jax.experimental.pallas import tpu as pltpu
from jax.sharding import PartitionSpec as P

TASKS = 8
SHARED = 8
MESH = pl.DeviceIdType.MESH


def flip(a, b, n):
    total, bit = 0, 1
    while bit < n:
        x, y = (a // bit) % 2, (b // bit) % 2
        total = total + bit * (x + y - 2 * x * y)
        bit *= 2
    return total


def each(lo, hi, fn):
    if hi - lo <= 16:
        for d in range(lo, hi):
            fn(d)
    else:

        @pl.loop(lo, hi)
        def _(d):
            fn(d)


def kernel(
    n,
    slot,
    room_ref,
    label_ref,
    sel_ref,
    mix_ref,
    x_ref,
    w1_hbm,
    w2_hbm,
    out_ref,
    w1,
    w2,
    outgoing,
    inbox,
    hidden,
    results,
    returned,
    counts,
    w_sem,
    send_sem,
    recv_sem,
    rsend_sem,
    rrecv_sem,
    csend_sem,
    crecv_sem,
):
    me = lax.axis_index("expert")
    group = lax.axis_index("groups")
    half = n // 2
    rows, width = x_ref.shape
    span = half * slot
    copies, task_width = n // (2 * SHARED), n // (2 * TASKS)

    load1 = pltpu.make_async_copy(w1_hbm.at[0], w1, w_sem.at[0])
    load2 = pltpu.make_async_copy(w2_hbm.at[0], w2, w_sem.at[1])
    load1.start()
    load2.start()

    barrier = pltpu.get_barrier_semaphore()

    def peer(d):
        return (group, flip(me, d, n))

    each(
        1,
        n,
        lambda d: pl.semaphore_signal(
            barrier, inc=1, device_id=peer(d), device_id_type=MESH
        ),
    )

    lane = lax.broadcasted_iota(jnp.int32, (1, rows), 1)
    task_id = SHARED * copies + label_ref[...] * task_width + sel_ref[0:1, :] - SHARED
    shared_id = sel_ref[1:2, :] * copies + lane % copies
    expert = lax.broadcasted_iota(jnp.int32, (n, rows), 0)
    hot = (expert == task_id) | (expert == shared_id)
    hot_f = hot.astype(jnp.float32)
    earlier = (
        lax.broadcasted_iota(jnp.int32, (rows, rows), 0)
        < lax.broadcasted_iota(jnp.int32, (rows, rows), 1)
    ).astype(jnp.float32)
    before = jnp.dot(
        hot_f.astype(jnp.bfloat16),
        earlier.astype(jnp.bfloat16),
        preferred_element_type=jnp.float32,
    )
    task_hot = (expert == task_id).astype(jnp.float32)
    shared_hot = (expert == shared_id).astype(jnp.float32)
    task_rank = jnp.sum(before * task_hot, axis=0, keepdims=True)
    shared_rank = jnp.sum(before * shared_hot, axis=0, keepdims=True)
    counts[0] = jnp.broadcast_to(jnp.sum(hot_f, axis=1, keepdims=True), (n, 128))

    task_slot = (task_id ^ me) * slot + task_rank.astype(jnp.int32)
    shared_slot = (shared_id ^ me) * slot + shared_rank.astype(jnp.int32)
    task_near = task_slot < span
    near_slot = jnp.where(task_near, task_slot, shared_slot)
    far_slot = jnp.where(task_near, shared_slot, task_slot) - span
    slot_row = lax.broadcasted_iota(jnp.int32, (span, rows), 0)

    def pack(slots):
        chosen = (slot_row == slots).astype(jnp.float32).astype(jnp.bfloat16)
        return jnp.dot(chosen, x_ref[...], preferred_element_type=jnp.float32).astype(
            jnp.bfloat16
        )

    def piece(ref, d):
        if isinstance(d, int):
            return ref.at[pl.ds(d * slot, slot)]
        return ref.at[pl.ds(pl.multiple_of(d * slot, slot), slot)]

    def dispatch(d):
        return pltpu.make_async_remote_copy(
            src_ref=piece(outgoing, d),
            dst_ref=piece(inbox, d),
            send_sem=send_sem.at[d],
            recv_sem=recv_sem.at[d],
            device_id=peer(d),
            device_id_type=MESH,
        )

    def answer(d):
        return pltpu.make_async_remote_copy(
            src_ref=piece(results, d),
            dst_ref=piece(returned, d),
            send_sem=rsend_sem.at[d],
            recv_sem=rrecv_sem.at[d],
            device_id=peer(d),
            device_id_type=MESH,
        )

    def tally(d):
        return pltpu.make_async_remote_copy(
            src_ref=counts.at[0],
            dst_ref=counts.at[d],
            send_sem=csend_sem.at[d],
            recv_sem=crecv_sem.at[d],
            device_id=peer(d),
            device_id_type=MESH,
        )

    outgoing[pl.ds(span, span)] = pack(far_slot)
    near_pack = pack(near_slot)
    outgoing[pl.ds(0, span)] = near_pack
    inbox[pl.ds(0, slot)] = near_pack[:slot]

    pl.semaphore_wait(barrier, n - 1)
    each(1, n, lambda d: dispatch(d).start())
    each(1, n, lambda d: tally(d).start())

    hid = w1.shape[1]
    tile = min(512, hid)
    out_tile = min(512, width)

    def mlp(first, size):
        @pl.loop(0, hid // tile)
        def _(t):
            cols = pl.ds(pl.multiple_of(t * tile, tile), tile)
            h = jnp.dot(
                inbox[pl.ds(first, size)],
                w1[:, cols],
                preferred_element_type=jnp.float32,
            )
            hidden[pl.ds(0, size), cols] = jax.nn.gelu(h).astype(jnp.bfloat16)

        @pl.loop(0, width // out_tile)
        def _(t):
            cols = pl.ds(pl.multiple_of(t * out_tile, out_tile), out_tile)
            y = jnp.dot(
                hidden[pl.ds(0, size)], w2[:, cols], preferred_element_type=jnp.float32
            )
            results[pl.ds(first, size), cols] = y.astype(jnp.bfloat16)

    load1.wait()
    load2.wait()
    each(1, half, lambda d: dispatch(d).wait_recv())
    mlp(0, span)
    each(1, half, lambda d: answer(d).start())
    returned[pl.ds(0, slot)] = results[pl.ds(0, slot)]

    quarter = half // 2
    for lo in (half, half + quarter):
        each(lo, lo + quarter, lambda d: dispatch(d).wait_recv())
        mlp(lo * slot, quarter * slot)
        each(lo, lo + quarter, lambda d: answer(d).start())

    each(1, n, lambda d: tally(d).wait_recv())

    offset = jnp.zeros((n, 128), jnp.float32)
    for d in range(1, n):
        source = flip(me, d, n)
        offset = offset + counts[d] * jnp.where(source < me, 1.0, 0.0)
    offset = offset[:, :1]
    arrival_task = task_rank + jnp.sum(task_hot * offset, axis=0, keepdims=True)
    arrival_shared = shared_rank + jnp.sum(shared_hot * offset, axis=0, keepdims=True)
    room_task = jnp.zeros((1, rows), jnp.int32)
    room_shared = jnp.zeros((1, rows), jnp.int32)
    for e in range(n):
        size = room_ref[e]
        if e < half:
            room_shared = jnp.where(shared_id == e, size, room_shared)
        else:
            room_task = jnp.where(task_id == e, size, room_task)
    keep_task = (arrival_task < room_task.astype(jnp.float32)).astype(jnp.float32)
    keep_shared = (arrival_shared < room_shared.astype(jnp.float32)).astype(jnp.float32)
    mix = mix_ref[...].astype(jnp.float32)
    total = mix[0:1] + mix[1:2]
    task_weight = mix[0:1] / total * keep_task
    shared_weight = mix[1:2] / total * keep_shared
    near_weight = jnp.where(task_near, task_weight, shared_weight)
    far_weight = jnp.where(task_near, shared_weight, task_weight)

    def column(row):
        return jnp.broadcast_to(row, (128, rows)).T[:, :1]

    near_column = column(near_slot.astype(jnp.float32))
    far_column = column(far_slot.astype(jnp.float32))
    near_weight = column(near_weight)
    far_weight = column(far_weight)
    slot_lane = lax.broadcasted_iota(jnp.int32, (rows, span), 1).astype(jnp.float32)

    def pick(slots, first):
        chosen = (slot_lane == slots).astype(jnp.float32).astype(jnp.bfloat16)
        return jnp.dot(
            chosen, returned[pl.ds(first, span)], preferred_element_type=jnp.float32
        )

    each(1, half, lambda d: answer(d).wait_recv())
    near = pick(near_column, 0) * near_weight
    each(half, n, lambda d: answer(d).wait_recv())
    out_ref[...] = (near + pick(far_column, span) * far_weight).astype(jnp.bfloat16)

    def drain(d):
        dispatch(d).wait_send()
        answer(d).wait_send()
        tally(d).wait_send()

    each(1, n, drain)


def solution(mesh):
    n = mesh.shape["expert"]

    def shards(x, label, sel, mix, room, first, second):
        rows, width = x.shape
        hid = first.shape[2]
        slot = -(-(4 * rows // n) // 16) * 16
        flat = pltpu.VMEM((n * slot, width), jnp.bfloat16)
        vmem = pl.BlockSpec(memory_space=pltpu.VMEM)
        anywhere = pl.BlockSpec(memory_space=pl.ANY)
        return pl.pallas_call(
            functools.partial(kernel, n, slot),
            out_shape=jax.ShapeDtypeStruct((rows, width), jnp.bfloat16),
            in_specs=[pl.BlockSpec(memory_space=pltpu.SMEM)]
            + [vmem] * 4
            + [anywhere] * 2,
            out_specs=vmem,
            scratch_shapes=[
                pltpu.VMEM(first.shape[1:], jnp.bfloat16),
                pltpu.VMEM(second.shape[1:], jnp.bfloat16),
                flat,
                flat,
                pltpu.VMEM((n * slot // 2, hid), jnp.bfloat16),
                flat,
                flat,
                pltpu.VMEM((n, n, 128), jnp.float32),
                pltpu.SemaphoreType.DMA((2,)),
            ]
            + [pltpu.SemaphoreType.DMA((n,))] * 6,
            compiler_params=pltpu.CompilerParams(
                collective_id=0, has_side_effects=True
            ),
        )(room, label.reshape(1, rows), sel.T, mix.T, x, first, second)

    in_specs = (
        P(("groups", "expert"), None),
        P(("groups", "expert")),
        P(("groups", "expert"), None),
        P(("groups", "expert"), None),
        P(),
        P("expert", None, None),
        P("expert", None, None),
    )
    return jax.shard_map(
        shards,
        mesh=mesh,
        in_specs=in_specs,
        out_specs=P(("groups", "expert"), None),
        check_vma=False,
    )
```

```python
import functools

import jax
import jax.numpy as jnp
from jax import lax
from jax.experimental import pallas as pl
from jax.experimental.pallas import tpu as pltpu
from jax.sharding import PartitionSpec as P

TASKS = 8
SHARED = 8
MESH = pl.DeviceIdType.MESH
CHUNKS = 4


def flip(a, b, n):
    total, bit = 0, 1
    while bit < n:
        x, y = (a // bit) % 2, (b // bit) % 2
        total = total + bit * (x + y - 2 * x * y)
        bit *= 2
    return total


def each(lo, hi, fn):
    if hi - lo <= 16:
        for d in range(lo, hi):
            fn(d)
    else:

        @pl.loop(lo, hi)
        def _(d):
            fn(d)


def kernel(
    n,
    slot,
    chunks,
    room_ref,
    label_ref,
    sel_ref,
    mix_ref,
    x_ref,
    w1_hbm,
    w2_hbm,
    out_ref,
    w1,
    w2,
    guests,
    outgoing,
    inbox,
    hidden,
    results,
    returned,
    home_out,
    home_in,
    partial,
    counts,
    route,
    w_sem,
    dense_sem,
    back_sem,
    route_sem,
    tally_send,
    tally_recv,
    near_send,
    near_recv,
    far_send,
    far_recv,
    near_rsend,
    near_rrecv,
    far_rsend,
    far_rrecv,
):
    me = lax.axis_index("expert")
    group = lax.axis_index("groups")
    half = n // 2
    rows, width = x_ref.shape
    span = half * slot
    part = width // chunks
    hid = w1.shape[1]
    padded = counts.shape[2]
    copies, task_width = n // (2 * SHARED), n // (2 * TASKS)

    load1 = pltpu.make_async_copy(w1_hbm.at[0], w1, w_sem.at[0])
    load2 = pltpu.make_async_copy(w2_hbm.at[0], w2, w_sem.at[1])
    load1.start()
    load2.start()

    barrier = pltpu.get_barrier_semaphore()

    def peer(d):
        return (group, flip(me, d, n))

    each(
        1,
        n,
        lambda d: pl.semaphore_signal(
            barrier, inc=1, device_id=peer(d), device_id_type=MESH
        ),
    )

    def remote(src, dst, send, recv, d):
        return pltpu.make_async_remote_copy(
            src_ref=src,
            dst_ref=dst,
            send_sem=send,
            recv_sem=recv,
            device_id=peer(d),
            device_id_type=MESH,
        )

    def block(first, d, k=None):
        start = first + d * slot
        if not isinstance(d, int):
            start = pl.multiple_of(start, slot)
        if k is None:
            return (pl.ds(start, slot), slice(None))
        return (pl.ds(start, slot), pl.ds(k * part, part))

    def columns(k):
        return (slice(None), pl.ds(k * part, part))

    def tally(d):
        return remote(
            counts.at[0], counts.at[d], tally_send.at[d], tally_recv.at[d], d
        )

    def plan():
        return remote(route.at[0], route.at[1], route_sem.at[0], route_sem.at[1], half)

    def dense(k):
        return remote(
            x_ref.at[columns(k)],
            guests.at[columns(k)],
            dense_sem.at[0, k],
            dense_sem.at[1, k],
            half,
        )

    def back(k):
        return remote(
            home_out.at[columns(k)],
            home_in.at[columns(k)],
            back_sem.at[0, k],
            back_sem.at[1, k],
            half,
        )

    def near_dispatch(d):
        at = block(0, d)
        return remote(outgoing.at[at], inbox.at[at], near_send.at[d], near_recv.at[d], d)

    def far_dispatch(d, k):
        at = block(span, d, k)
        return remote(
            outgoing.at[at], inbox.at[at], far_send.at[d, k], far_recv.at[d, k], d
        )

    def near_answer(d):
        at = block(0, d)
        return remote(
            results.at[at], returned.at[at], near_rsend.at[d], near_rrecv.at[d], d
        )

    def far_answer(d, k):
        at = block(span, d, k)
        return remote(
            results.at[at], returned.at[at], far_rsend.at[d, k], far_rrecv.at[d, k], d
        )

    lane = lax.broadcasted_iota(jnp.int32, (1, rows), 1)
    task_id = SHARED * copies + label_ref[...] * task_width + sel_ref[0:1, :] - SHARED
    shared_id = sel_ref[1:2, :] * copies + lane % copies
    expert = lax.broadcasted_iota(jnp.int32, (padded, rows), 0)
    task_hot = (expert == task_id).astype(jnp.float32)
    shared_hot = (expert == shared_id).astype(jnp.float32)
    hot = (task_hot + shared_hot).astype(jnp.bfloat16)
    earlier = (
        lax.broadcasted_iota(jnp.int32, (rows, rows), 0)
        < lax.broadcasted_iota(jnp.int32, (rows, rows), 1)
    ).astype(jnp.float32)
    before = jnp.dot(
        hot, earlier.astype(jnp.bfloat16), preferred_element_type=jnp.float32
    )
    task_rank = jnp.sum(before * task_hot, axis=0, keepdims=True)
    shared_rank = jnp.sum(before * shared_hot, axis=0, keepdims=True)
    counts[0] = lax.dot_general(
        jnp.ones((8, rows), jnp.bfloat16),
        hot,
        (((1,), (1,)), ((), ())),
        preferred_element_type=jnp.float32,
    )[:1]

    task_slot = (task_id ^ me) * slot + task_rank.astype(jnp.int32)
    shared_slot = (shared_id ^ me) * slot + shared_rank.astype(jnp.int32)
    task_near = task_slot < span
    near_slot = jnp.where(task_near, task_slot, shared_slot)
    far_slot = jnp.where(task_near, shared_slot, task_slot) - span
    route[0] = far_slot
    slot_row = lax.broadcasted_iota(jnp.int32, (span, rows), 0)

    def choice(slots):
        return (slot_row == slots).astype(jnp.float32).astype(jnp.bfloat16)

    def pack(chosen, block_rows):
        return jnp.dot(chosen, block_rows, preferred_element_type=jnp.float32).astype(
            jnp.bfloat16
        )

    near_pack = pack(choice(near_slot), x_ref[...])
    outgoing[pl.ds(0, span)] = near_pack
    inbox[pl.ds(0, slot)] = near_pack[:slot]

    pl.semaphore_wait(barrier, n - 1)
    plan().start()
    for k in range(chunks):
        dense(k).start()
    each(1, n, lambda d: tally(d).start())
    each(1, half, lambda d: near_dispatch(d).start())

    plan().wait_recv()
    guest_slot = route[1]
    guest_choice = choice(guest_slot)
    for k in range(chunks):
        dense(k).wait_recv()
        packed = pack(guest_choice, guests[columns(k)])
        outgoing[pl.ds(span, span), pl.ds(k * part, part)] = packed
        inbox[pl.ds(span, slot), pl.ds(k * part, part)] = packed[:slot]
        each(1, half, lambda d: far_dispatch(d, k).start())

    tile = min(512, hid)

    def expand(first):
        @pl.loop(0, hid // tile)
        def _(t):
            cols = pl.ds(pl.multiple_of(t * tile, tile), tile)
            h = jnp.dot(
                inbox[pl.ds(first, span)],
                w1[:, cols],
                preferred_element_type=jnp.float32,
            )
            hidden[:, cols] = jax.nn.gelu(h).astype(jnp.bfloat16)

    def shrink(first, cols):
        y = jnp.dot(hidden[...], w2[:, cols], preferred_element_type=jnp.float32)
        results[pl.ds(first, span), cols] = y.astype(jnp.bfloat16)

    load1.wait()
    load2.wait()
    each(1, half, lambda d: near_dispatch(d).wait_recv())
    expand(0)

    out_tile = min(512, width)

    @pl.loop(0, width // out_tile)
    def _(t):
        shrink(0, pl.ds(pl.multiple_of(t * out_tile, out_tile), out_tile))

    each(1, half, lambda d: near_answer(d).start())
    returned[pl.ds(0, slot)] = results[pl.ds(0, slot)]

    for k in range(chunks):
        each(1, half, lambda d: far_dispatch(d, k).wait_recv())
    expand(span)
    for k in range(chunks):
        shrink(span, pl.ds(k * part, part))
        each(1, half, lambda d: far_answer(d, k).start())
        own = (pl.ds(span, slot), pl.ds(k * part, part))
        returned[own] = results[own]

    each(1, n, lambda d: tally(d).wait_recv())

    def column(row):
        return jnp.broadcast_to(row, (128, row.shape[1])).T[:, :1]

    offset = jnp.zeros((1, padded), jnp.float32)
    for d in range(1, n):
        offset = offset + counts[d] * jnp.where(flip(me, d, n) < me, 1.0, 0.0)
    offset = column(offset)
    arrival_task = task_rank + jnp.sum(task_hot * offset, axis=0, keepdims=True)
    arrival_shared = shared_rank + jnp.sum(shared_hot * offset, axis=0, keepdims=True)
    room_task = jnp.zeros((1, rows), jnp.int32)
    room_shared = jnp.zeros((1, rows), jnp.int32)
    for e in range(n):
        size = room_ref[e]
        if e < half:
            room_shared = jnp.where(shared_id == e, size, room_shared)
        else:
            room_task = jnp.where(task_id == e, size, room_task)
    keep_task = (arrival_task < room_task.astype(jnp.float32)).astype(jnp.float32)
    keep_shared = (arrival_shared < room_shared.astype(jnp.float32)).astype(jnp.float32)
    mix = mix_ref[...].astype(jnp.float32)
    total = mix[0:1] + mix[1:2]
    task_weight = mix[0:1] / total * keep_task
    shared_weight = mix[1:2] / total * keep_shared
    near_weight = column(jnp.where(task_near, task_weight, shared_weight))
    far_weight = column(jnp.where(task_near, shared_weight, task_weight))
    slot_lane = lax.broadcasted_iota(jnp.int32, (rows, span), 1).astype(jnp.float32)

    def reader(slots):
        slots = column(slots.astype(jnp.float32))
        return (slot_lane == slots).astype(jnp.float32).astype(jnp.bfloat16)

    near_reader = reader(near_slot)
    guest_reader = reader(guest_slot)

    each(1, half, lambda d: near_answer(d).wait_recv())
    partial[...] = (
        jnp.dot(
            near_reader, returned[pl.ds(0, span)], preferred_element_type=jnp.float32
        )
        * near_weight
    )

    for k in range(chunks):
        each(1, half, lambda d: far_answer(d, k).wait_recv())
        home_out[columns(k)] = pack(
            guest_reader, returned[pl.ds(span, span), pl.ds(k * part, part)]
        )
        back(k).start()

    for k in range(chunks):
        back(k).wait_recv()
        out_ref[columns(k)] = (
            partial[columns(k)] + home_in[columns(k)].astype(jnp.float32) * far_weight
        ).astype(jnp.bfloat16)

    plan().wait_send()
    each(1, n, lambda d: tally(d).wait_send())
    for k in range(chunks):
        dense(k).wait_send()
        back(k).wait_send()

    def drain(d):
        near_dispatch(d).wait_send()
        near_answer(d).wait_send()
        for k in range(chunks):
            far_dispatch(d, k).wait_send()
            far_answer(d, k).wait_send()

    each(1, half, drain)


def solution(mesh):
    n = mesh.shape["expert"]

    def shards(x, label, sel, mix, room, first, second):
        rows, width = x.shape
        hid = first.shape[2]
        slot = -(-(4 * rows // n) // 16) * 16
        chunks = CHUNKS
        half = n // 2
        padded = -(-n // 128) * 128
        flat = pltpu.VMEM((n * slot, width), jnp.bfloat16)
        plain = pltpu.VMEM((rows, width), jnp.bfloat16)
        vmem = pl.BlockSpec(memory_space=pltpu.VMEM)
        anywhere = pl.BlockSpec(memory_space=pl.ANY)
        dma = pltpu.SemaphoreType.DMA
        return pl.pallas_call(
            functools.partial(kernel, n, slot, chunks),
            out_shape=jax.ShapeDtypeStruct((rows, width), jnp.bfloat16),
            in_specs=[pl.BlockSpec(memory_space=pltpu.SMEM)]
            + [vmem] * 4
            + [anywhere] * 2,
            out_specs=vmem,
            scratch_shapes=[
                pltpu.VMEM(first.shape[1:], jnp.bfloat16),
                pltpu.VMEM(second.shape[1:], jnp.bfloat16),
                plain,
                flat,
                flat,
                pltpu.VMEM((half * slot, hid), jnp.bfloat16),
                flat,
                flat,
                plain,
                plain,
                pltpu.VMEM((rows, width), jnp.float32),
                pltpu.VMEM((n, 1, padded), jnp.float32),
                pltpu.VMEM((2, 1, rows), jnp.int32),
                dma((2,)),
                dma((2, chunks)),
                dma((2, chunks)),
                dma((2,)),
                dma((n,)),
                dma((n,)),
                dma((half,)),
                dma((half,)),
                dma((half, chunks)),
                dma((half, chunks)),
                dma((half,)),
                dma((half,)),
                dma((half, chunks)),
                dma((half, chunks)),
            ],
            compiler_params=pltpu.CompilerParams(
                collective_id=0, has_side_effects=True
            ),
        )(room, label.reshape(1, rows), sel.T, mix.T, x, first, second)

    in_specs = (
        P(("groups", "expert"), None),
        P(("groups", "expert")),
        P(("groups", "expert"), None),
        P(("groups", "expert"), None),
        P(),
        P("expert", None, None),
        P("expert", None, None),
    )
    return jax.shard_map(
        shards,
        mesh=mesh,
        in_specs=in_specs,
        out_specs=P(("groups", "expert"), None),
        check_vma=False,
    )
```
